128 devices in a mesh: items: 32 (over y, z, core), users: 4 (over x).
Axes of the slice: x: 4, y: 4, z: 4, core: 2. Of those that a mesh axis runs over, the one named last changes fastest.
Arguments:
- user_emb: bfloat16 [4096, 256], P('users', 'items'), as said below
- item_emb: bfloat16 [1048576, 256], P('items'), as said below
- target: int32 [4096], P('users'), may hold values from 0 to 1048575
- history: int32 [4096, 32], P('users'), may hold values from 0 to 1048575, as said below
Outputs:
- log_rank: float32 [4096], P('users')
- metrics: float32 [2], replicated
The draws below stay inside these ranges and needn't reach their ends.
Inputs may be any that keep to these rules, and one draw needn't show every extreme that they name: history[u, k] lies in [k * 32768, (k + 1) * 32768); a user's history entries are thus distinct. `item_emb`: rows of norm about one. `user_emb`: entries of order one.
All inputs are finite; a program needn't handle non-finite values.
Results may differ from the reference program's by a relative error of at most 0.0003.
Values may be sent and summed in bfloat16 or wider, within the bound.
No kernel may reach another device: no remote copies, remote signals or barrier semaphores. Data moves between devices by JAX's collectives and lax.ppermute only.
A program may use at most 64 MiB of HBM per device.

```python
import jax
import jax.numpy as jnp
from jax import lax

D = 256
H = 32
ITEMS = 1048576
USERS = 4096


def item_row(base, row):
    return jax.random.normal(jax.random.fold_in(base, row), (D,), jnp.float32) / jnp.sqrt(float(D))


def shared_ints(key):
    target = jax.random.randint(jax.random.fold_in(key, 12), (USERS,), 0, ITEMS).astype(jnp.int32)
    stride = ITEMS // H
    offset = jax.random.randint(jax.random.fold_in(key, 13), (USERS, H), 0, stride).astype(jnp.int32)
    history = offset + (jnp.arange(H, dtype=jnp.int32) * stride)[None, :]
    return (target, history)


def draw_item_emb(key, part):
    base = jax.random.fold_in(key, 11)
    rows = jax.vmap(lambda r: item_row(base, r))(jnp.arange(ITEMS, dtype=jnp.int32))
    return rows.astype(jnp.bfloat16)


def draw_target(key, part):
    return shared_ints(key)[0]


def draw_history(key, part):
    return shared_ints(key)[1]


def draw_user_emb(key, part):
    base = jax.random.fold_in(key, 11)
    target, history = shared_ints(key)
    trow = jax.vmap(lambda r: item_row(base, r))(target)
    hrows = jax.vmap(jax.vmap(lambda r: item_row(base, r)))(history)
    noise = jax.random.normal(jax.random.fold_in(key, 14), (USERS, D), jnp.float32) * 0.6
    query = noise + 4.0 * trow + 2.5 * jnp.sum(hrows, axis=1)
    return query.astype(jnp.bfloat16)


def setup_inputs(seed: int = 0) -> dict:
    key_of = jax.random.split(jax.random.key(seed), 5)
    return {
        "user_emb": draw_user_emb(jax.random.fold_in(key_of[4], 71), 0),
        "item_emb": draw_item_emb(jax.random.fold_in(key_of[4], 71), 0),
        "target": draw_target(jax.random.fold_in(key_of[4], 71), 0),
        "history": draw_history(jax.random.fold_in(key_of[4], 71), 0),
    }


sharpness = 4.0


def reference(user_emb, item_emb, target, history):
    users = user_emb.astype(jnp.float32)
    items = item_emb.astype(jnp.float32)
    tscore = jnp.sum(users * items[target], axis=1)
    blk = min(ITEMS, 8192)
    nblk = ITEMS // blk
    blocks = items.reshape(nblk, blk, D)

    def step(total, rows):
        score = jnp.dot(users, rows.T, preferred_element_type=jnp.float32, precision=lax.Precision.HIGHEST)
        return total + jnp.sum(jax.nn.sigmoid(sharpness * (score - tscore[:, None])), axis=1), None

    total, _ = lax.scan(step, jnp.zeros((USERS,), jnp.float32), blocks)
    hrows = items[history]
    hscore = jnp.einsum("ud,uhd->uh", users, hrows, precision=lax.Precision.HIGHEST)
    seen_sum = jnp.sum(jax.nn.sigmoid(sharpness * (hscore - tscore[:, None])), axis=1)
    seen = jnp.any(history == target[:, None], axis=1)
    above = total - seen_sum - jnp.where(seen, 0.0, 0.5).astype(jnp.float32)
    rank = 1.0 + above
    log_rank = jnp.log(rank)
    hit = jax.nn.sigmoid(10.5 - rank)
    gain = hit / jnp.log2(1.0 + rank)
    metrics = jnp.stack([jnp.sum(hit), jnp.sum(gain)]) / USERS
    return log_rank, metrics
```

```python
import functools

import jax
import jax.numpy as jnp
from jax import lax
from jax.experimental import pallas as pl
from jax.experimental.pallas import tpu as pltpu
from jax.sharding import PartitionSpec as P

sharpness = 4.0
block_items = 4096
chunk_items = 256
chunk_users = 512
largest = 1e37


def gather_kernel(tidx, hidx, tkey, hkey, target, history, items, trow, hrow, fix, tbuf, hbuf, tsem, hsem):
    u_dev = tkey.shape[1]

    def start(u, _):
        r = pl.multiple_of((tidx[u] >> 3) * 8, 8)
        pltpu.make_async_copy(items.at[pl.ds(r, 8), :], tbuf.at[u], tsem).start()
        r = pl.multiple_of((hidx[u] >> 3) * 8, 8)
        pltpu.make_async_copy(items.at[pl.ds(r, 8), :], hbuf.at[u], hsem).start()
        return 0

    lax.fori_loop(0, u_dev, start, 0, unroll=8)
    seen = jnp.any(history[...] == target[...], axis=0, keepdims=True)
    fix[...] = jnp.where(seen, 0.0, 0.5).astype(jnp.float32)
    n = 256
    for idx, key, buf, sem, out in ((tidx, tkey, tbuf, tsem, trow), (hidx, hkey, hbuf, hsem, hrow)):
        pltpu.make_async_copy(buf, buf, sem).wait()
        for b in range(u_dev // n):
            rows = buf[b * n : (b + 1) * n].reshape(n * 8, buf.shape[2])
            at = lax.broadcasted_iota(jnp.int32, (n * 8, n), 0)
            own = lax.broadcasted_iota(jnp.int32, (1, n), 1) * 8 + (key[:, b * n : (b + 1) * n] & 7)
            pick = jnp.where(at == own, 1.0, 0.0).astype(jnp.bfloat16)
            out[:, b * n : (b + 1) * n] = lax.dot_general(
                rows, pick, (((0,), (0,)), ((), ())), preferred_element_type=jnp.float32
            ).astype(jnp.bfloat16)


def tscore_kernel(users, trow, inside, out):
    prod = users[...].astype(jnp.float32) * trow[...].astype(jnp.float32)
    part = jnp.where(inside[...] > 0, jnp.sum(prod, axis=0, keepdims=True), 0.0)
    out[...] = jnp.broadcast_to(part[None], out.shape)


def count_kernel(users, hrow, parts, block, items, out, scaled, total, far, tscore, buf, sem):
    step = pl.program_id(0)
    u_dev = users.shape[1]

    @pl.when(step == 0)
    def _():
        total[...] = jnp.zeros_like(total)
        far[...] = jnp.zeros_like(far)
        tscore[...] = jnp.sum(parts[...], axis=0)
        scaled[...] = users[...] * jnp.bfloat16(-sharpness)

    for n in range(u_dev // chunk_users):
        cols = slice(n * chunk_users, (n + 1) * chunk_users)
        w = scaled[:, cols]
        base = jnp.exp(-sharpness * tscore[:, cols])
        acc = total[:, cols]
        top = far[:, cols]
        for c in range(block_items // chunk_items):
            x = jnp.dot(
                block[c * chunk_items : (c + 1) * chunk_items, :], w, preferred_element_type=jnp.float32
            )
            d = (jnp.exp(x) + base).reshape(chunk_items // 16, 2, 8, chunk_users)
            both = d[:, 0] * d[:, 1]
            acc = acc + jnp.sum((d[:, 0] + d[:, 1]) * (1.0 / both), axis=0)
            top = jnp.maximum(top, jnp.max(both, axis=0))
        total[:, cols] = acc
        far[:, cols] = top

    @pl.when(step == pl.num_programs(0) - 1)
    def _():
        ts = tscore[...]
        base = jnp.exp(-sharpness * ts)
        count = jnp.sum(total[...], axis=0, keepdims=True) * base
        good = (jnp.max(far[...], axis=0, keepdims=True) < largest) & (jnp.abs(sharpness * ts) < 60.0)
        good = good & (count < largest)
        hscore = jnp.sum(users[...].astype(jnp.float32) * hrow[...].astype(jnp.float32), axis=0, keepdims=True)
        taken = 1.0 / (1.0 + jnp.exp(jnp.minimum(sharpness * (ts - hscore), 80.0)))
        out[...] = jnp.broadcast_to((count - taken)[None], out.shape)
        bad = jnp.sum(jnp.where(good, 0.0, 1.0))

        @pl.when(bad > 0.0)
        def _():
            total[...] = jnp.zeros_like(total)

            def again(i, _):
                copy = pltpu.make_async_copy(items.at[pl.ds(i * 256, 256), :], buf, sem)
                copy.start()
                copy.wait()
                for n in range(u_dev // 256):
                    cols = slice(n * 256, (n + 1) * 256)
                    s = jnp.dot(buf[...], users[:, cols], preferred_element_type=jnp.float32)
                    x = jnp.minimum(sharpness * (tscore[:, cols] - s), 80.0)
                    total[:, cols] += jnp.sum((1.0 / (1.0 + jnp.exp(x))).reshape(32, 8, 256), axis=0)
                return 0

            lax.fori_loop(0, items.shape[0] // 256, again, 0)
            exact = jnp.sum(total[...], axis=0, keepdims=True)
            out[...] = jnp.broadcast_to((exact - taken)[None], out.shape)


def metric_kernel(parts, fix, log_rank, sums):
    above = jnp.sum(parts[...], axis=0) - fix[...]
    rank = 1.0 + above
    log_rank[...] = jnp.log(rank)
    hit = 1.0 / (1.0 + jnp.exp(rank - 10.5))
    gain = hit / (jnp.log(1.0 + rank) * (1.0 / 0.6931471805599453))
    lane = lax.broadcasted_iota(jnp.int32, (1, 128), 1)
    row = jnp.where(lane == 0, jnp.sum(hit), jnp.where(lane == 1, jnp.sum(gain), 0.0))
    sums[...] = jnp.broadcast_to(row[None], sums.shape)


def body(user_emb, item_emb, target, history):
    item_dev, dim = item_emb.shape
    u_dev = user_emb.shape[0]
    n_items = lax.axis_size("items")
    n_users = lax.axis_size("users")
    shard = lax.axis_index("items")
    start = shard * item_dev
    f32 = jnp.float32
    vmem = pl.BlockSpec(memory_space=pltpu.VMEM)
    smem = pl.BlockSpec(memory_space=pltpu.SMEM)
    hbm = pl.BlockSpec(memory_space=pl.ANY)
    big = pltpu.CompilerParams(vmem_limit_bytes=56 * 1024 * 1024)

    columns = jnp.broadcast_to(user_emb.T[None], (n_items, dim // n_items, u_dev))
    users = lax.all_to_all(columns, "items", split_axis=0, concat_axis=0, tiled=True).reshape(dim, u_dev)

    local_t = target - start
    inside = ((local_t >= 0) & (local_t < item_dev)).astype(f32)[None]
    tidx = jnp.clip(local_t, 0, item_dev - 1)
    hidx = lax.dynamic_slice_in_dim(history.T, shard, 1, 0)[0] - start
    trow, hrow, fix = pl.pallas_call(
        gather_kernel,
        out_shape=(
            jax.ShapeDtypeStruct((dim, u_dev), jnp.bfloat16),
            jax.ShapeDtypeStruct((dim, u_dev), jnp.bfloat16),
            jax.ShapeDtypeStruct((1, u_dev), f32),
        ),
        in_specs=[smem, smem, vmem, vmem, vmem, vmem, hbm],
        out_specs=(vmem, vmem, vmem),
        scratch_shapes=[
            pltpu.VMEM((u_dev, 8, dim), jnp.bfloat16),
            pltpu.VMEM((u_dev, 8, dim), jnp.bfloat16),
            pltpu.SemaphoreType.DMA,
            pltpu.SemaphoreType.DMA,
        ],
        compiler_params=big,
        name="gather",
    )(tidx, hidx, tidx[None], hidx[None], target[None], history.T, item_emb)

    spread = jax.ShapeDtypeStruct((n_items, 1, u_dev), f32)
    part_t = pl.pallas_call(
        tscore_kernel, out_shape=spread, in_specs=[vmem] * 3, out_specs=vmem, name="tscore"
    )(users, trow, inside)
    parts_t = lax.all_to_all(part_t, "items", split_axis=0, concat_axis=0, tiled=True)

    whole = lambda a: pl.BlockSpec(a.shape, lambda i: (0,) * len(a.shape))
    local = pl.pallas_call(
        count_kernel,
        grid=(item_dev // block_items,),
        out_shape=spread,
        in_specs=[
            whole(users),
            whole(hrow),
            whole(parts_t),
            pl.BlockSpec((block_items, dim), lambda i: (i, 0)),
            hbm,
        ],
        out_specs=pl.BlockSpec(spread.shape, lambda i: (0, 0, 0)),
        scratch_shapes=[
            pltpu.VMEM((dim, u_dev), jnp.bfloat16),
            pltpu.VMEM((8, u_dev), f32),
            pltpu.VMEM((8, u_dev), f32),
            pltpu.VMEM((1, u_dev), f32),
            pltpu.VMEM((256, dim), jnp.bfloat16),
            pltpu.SemaphoreType.DMA,
        ],
        compiler_params=pltpu.CompilerParams(
            vmem_limit_bytes=56 * 1024 * 1024,
        ),
        name="count",
    )(users, hrow, parts_t, item_emb, item_emb)

    parts = lax.all_to_all(local, "items", split_axis=0, concat_axis=0, tiled=True)
    log_rank, sums = pl.pallas_call(
        metric_kernel,
        out_shape=(jax.ShapeDtypeStruct((1, u_dev), f32), jax.ShapeDtypeStruct((n_users, 1, 128), f32)),
        in_specs=[vmem, vmem],
        out_specs=(vmem, vmem),
        name="metric",
    )(parts, fix)
    sums = lax.all_to_all(sums, "users", split_axis=0, concat_axis=0, tiled=True)
    metrics = jnp.sum(sums, axis=(0, 1))[:2] / (u_dev * n_users)
    return (log_rank[0], metrics)


def solution(mesh):
    return jax.shard_map(
        body,
        mesh=mesh,
        in_specs=(P("users", "items"), P("items", None), P("users"), P("users", None)),
        out_specs=(P("users"), P()),
        check_vma=False,
    )
```

```python
import functools

import jax
import jax.numpy as jnp
from jax import lax
from jax.experimental import pallas as pl
from jax.experimental.pallas import tpu as pltpu
from jax.sharding import PartitionSpec as P

sharpness = 4.0
block_items = 4096
chunk_items = 512
chunk_users = 256
largest = 1e37


def spread_kernel(own, out, sem):
    for i in range(out.shape[0]):
        pltpu.make_async_copy(own, out.at[i], sem).start()
    pltpu.make_async_copy(out, out, sem).wait()


def gather_kernel(tscalar, target, history, hist_hbm, items, trow, hrow, fix, hscalar, tbuf, hbuf, ssem, tsem, hsem):
    u_dev = target.shape[1]
    item_dev = items.shape[0]
    shard = lax.axis_index("items")
    first = shard * item_dev
    group = (shard >> 3) * 8
    row = shard - group
    mine = pltpu.make_async_copy(hist_hbm.at[pl.ds(pl.multiple_of(group, 8), 8), :], hscalar, ssem)
    mine.start()

    def start_t(u, _):
        r = pl.multiple_of((lax.rem(tscalar[u], item_dev) >> 3) * 8, 8)
        pltpu.make_async_copy(items.at[pl.ds(r, 8), :], tbuf.at[u], tsem).start()
        return 0

    def start_h(u, _):
        r = pl.multiple_of(((hscalar[row, u] - first) >> 3) * 8, 8)
        pltpu.make_async_copy(items.at[pl.ds(r, 8), :], hbuf.at[u], hsem).start()
        return 0

    lax.fori_loop(0, u_dev, start_t, 0, unroll=16)
    mine.wait()
    lax.fori_loop(0, u_dev, start_h, 0, unroll=16)
    seen = jnp.any(history[...] == target[...], axis=0, keepdims=True)
    fix[...] = jnp.where(seen, 0.0, 0.5).astype(jnp.float32)
    own_hist = history[pl.ds(shard, 1), :]
    n = 128
    at = lax.broadcasted_iota(jnp.int32, (n * 8, n), 0)
    lane = lax.broadcasted_iota(jnp.int32, (1, n), 1) * 8
    for key, buf, sem, out in ((target[...], tbuf, tsem, trow), (own_hist, hbuf, hsem, hrow)):
        pltpu.make_async_copy(buf, buf, sem).wait()
        for b in range(u_dev // n):
            rows = buf[b * n : (b + 1) * n].reshape(n * 8, buf.shape[2])
            own = lane + (key[:, b * n : (b + 1) * n] & 7)
            pick = jnp.where(at == own, 1.0, 0.0).astype(jnp.bfloat16)
            out[:, b * n : (b + 1) * n] = lax.dot_general(
                rows, pick, (((0,), (0,)), ((), ())), preferred_element_type=jnp.float32
            ).astype(jnp.bfloat16)


def tscore_kernel(users, trow, target, out, *, item_dev):
    local = target[...] - lax.axis_index("items") * item_dev
    prod = users[...].astype(jnp.float32) * trow[...].astype(jnp.float32)
    part = jnp.where((local >= 0) & (local < item_dev), jnp.sum(prod, axis=0, keepdims=True), 0.0)
    out[...] = jnp.broadcast_to(part[None], out.shape)


def count_kernel(users, hrow, parts, items, out, block, scaled, total, far, tscore, sems):
    u_dev = users.shape[1]
    n_blocks = items.shape[0] // block_items

    def fetch(i):
        at = pl.ds(pl.multiple_of(i * block_items, block_items), block_items)
        return pltpu.make_async_copy(items.at[at, :], block.at[lax.rem(i, 3)], sems.at[lax.rem(i, 3)])

    fetch(0).start()
    fetch(1).start()
    total[...] = jnp.zeros_like(total)
    far[...] = jnp.zeros_like(far)
    ts = jnp.sum(parts[...], axis=0)
    tscore[...] = ts
    scaled[...] = users[...] * jnp.bfloat16(-sharpness)
    hscore = jnp.sum(users[...].astype(jnp.float32) * hrow[...].astype(jnp.float32), axis=0, keepdims=True)
    taken = 1.0 / (1.0 + jnp.exp(jnp.minimum(sharpness * (ts - hscore), 80.0)))

    def step(i, _):
        @pl.when(i + 2 < n_blocks)
        def _():
            fetch(i + 2).start()

        fetch(i).wait()
        slot = lax.rem(i, 3)
        for n in range(u_dev // chunk_users):
            cols = slice(n * chunk_users, (n + 1) * chunk_users)
            w = scaled[:, cols]
            base = jnp.exp(-sharpness * tscore[:, cols])
            acc = total[:, cols]
            top = far[:, cols]
            for c in range(block_items // chunk_items):
                x = jnp.dot(
                    block[slot, c * chunk_items : (c + 1) * chunk_items, :], w, preferred_element_type=jnp.float32
                )
                d = (jnp.exp(x) + base).reshape(chunk_items // 16, 2, 8, chunk_users)
                both = d[:, 0] * d[:, 1]
                acc = acc + jnp.sum((d[:, 0] + d[:, 1]) * (1.0 / both), axis=0)
                top = jnp.maximum(top, jnp.max(both, axis=0))
            total[:, cols] = acc
            far[:, cols] = top
        return 0

    lax.fori_loop(0, n_blocks, step, 0)
    base = jnp.exp(-sharpness * ts)
    count = jnp.sum(total[...], axis=0, keepdims=True) * base
    good = (jnp.max(far[...], axis=0, keepdims=True) < largest) & (jnp.abs(sharpness * ts) < 60.0)
    good = good & (count < largest)
    out[...] = jnp.broadcast_to((count - taken)[None], out.shape)
    bad = jnp.sum(jnp.where(good, 0.0, 1.0))

    @pl.when(bad > 0.0)
    def _():
        total[...] = jnp.zeros_like(total)

        def again(i, _):
            rows = pl.ds(pl.multiple_of(i * 256, 256), 256)
            copy = pltpu.make_async_copy(items.at[rows, :], block.at[0, pl.ds(0, 256), :], sems.at[0])
            copy.start()
            copy.wait()
            for n in range(u_dev // 256):
                cols = slice(n * 256, (n + 1) * 256)
                s = jnp.dot(block[0, :256, :], users[:, cols], preferred_element_type=jnp.float32)
                x = jnp.minimum(sharpness * (tscore[:, cols] - s), 80.0)
                total[:, cols] += jnp.sum((1.0 / (1.0 + jnp.exp(x))).reshape(32, 8, 256), axis=0)
            return 0

        lax.fori_loop(0, items.shape[0] // 256, again, 0)
        exact = jnp.sum(total[...], axis=0, keepdims=True)
        out[...] = jnp.broadcast_to((exact - taken)[None], out.shape)


def metric_kernel(parts, fix, log_rank, sums):
    above = jnp.sum(parts[...], axis=0) - fix[...]
    rank = 1.0 + above
    log_rank[...] = jnp.log(rank)
    hit = 1.0 / (1.0 + jnp.exp(rank - 10.5))
    gain = hit / (jnp.log(1.0 + rank) * (1.0 / 0.6931471805599453))
    lane = lax.broadcasted_iota(jnp.int32, (1, 128), 1)
    row = jnp.where(lane == 0, jnp.sum(hit), jnp.where(lane == 1, jnp.sum(gain), 0.0))
    sums[...] = jnp.broadcast_to(row[None], sums.shape)


def body(user_emb, item_emb, target, history):
    item_dev, dim = item_emb.shape
    u_dev = user_emb.shape[0]
    n_items = lax.axis_size("items")
    n_users = lax.axis_size("users")
    f32 = jnp.float32
    vmem = pl.BlockSpec(memory_space=pltpu.VMEM)
    smem = pl.BlockSpec(memory_space=pltpu.SMEM)
    hbm = pl.BlockSpec(memory_space=pl.ANY)

    small = pltpu.CompilerParams(vmem_limit_bytes=8 * 1024 * 1024)
    columns = pl.pallas_call(
        spread_kernel,
        out_shape=jax.ShapeDtypeStruct((n_items, dim // n_items, u_dev), jnp.bfloat16),
        in_specs=[vmem],
        out_specs=hbm,
        scratch_shapes=[pltpu.SemaphoreType.DMA],
        compiler_params=small,
        name="spread",
    )(user_emb.T)
    users = lax.all_to_all(columns, "items", split_axis=0, concat_axis=0, tiled=True).reshape(dim, u_dev)

    trow, hrow, fix = pl.pallas_call(
        gather_kernel,
        out_shape=(
            jax.ShapeDtypeStruct((dim, u_dev), jnp.bfloat16),
            jax.ShapeDtypeStruct((dim, u_dev), jnp.bfloat16),
            jax.ShapeDtypeStruct((1, u_dev), f32),
        ),
        in_specs=[smem, vmem, vmem, hbm, hbm],
        out_specs=(vmem, vmem, vmem),
        scratch_shapes=[
            pltpu.SMEM((8, u_dev), jnp.int32),
            pltpu.VMEM((u_dev, 8, dim), jnp.bfloat16),
            pltpu.VMEM((u_dev, 8, dim), jnp.bfloat16),
            pltpu.SemaphoreType.DMA,
            pltpu.SemaphoreType.DMA,
            pltpu.SemaphoreType.DMA,
        ],
        compiler_params=pltpu.CompilerParams(vmem_limit_bytes=40 * 1024 * 1024),
        name="gather",
    )(target, target[None], history.T, history.T, item_emb)

    spread = jax.ShapeDtypeStruct((n_items, 1, u_dev), f32)
    part_t = pl.pallas_call(
        functools.partial(tscore_kernel, item_dev=item_dev),
        out_shape=spread,
        in_specs=[vmem] * 3,
        out_specs=vmem,
        compiler_params=small,
        name="tscore",
    )(users, trow, target[None])
    parts_t = lax.all_to_all(part_t, "items", split_axis=0, concat_axis=0, tiled=True)

    local = pl.pallas_call(
        count_kernel,
        out_shape=spread,
        in_specs=[vmem, vmem, vmem, hbm],
        out_specs=vmem,
        scratch_shapes=[
            pltpu.VMEM((3, block_items, dim), jnp.bfloat16),
            pltpu.VMEM((dim, u_dev), jnp.bfloat16),
            pltpu.VMEM((8, u_dev), f32),
            pltpu.VMEM((8, u_dev), f32),
            pltpu.VMEM((1, u_dev), f32),
            pltpu.SemaphoreType.DMA((3,)),
        ],
        compiler_params=pltpu.CompilerParams(
            vmem_limit_bytes=40 * 1024 * 1024,
        ),
        name="count",
    )(users, hrow, parts_t, item_emb)

    parts = lax.all_to_all(local, "items", split_axis=0, concat_axis=0, tiled=True)
    log_rank, sums = pl.pallas_call(
        metric_kernel,
        out_shape=(jax.ShapeDtypeStruct((1, u_dev), f32), jax.ShapeDtypeStruct((n_users, 1, 128), f32)),
        in_specs=[vmem, vmem],
        out_specs=(vmem, vmem),
        compiler_params=small,
        name="metric",
    )(parts, fix)
    sums = lax.all_to_all(sums, "users", split_axis=0, concat_axis=0, tiled=True)
    metrics = jnp.sum(sums, axis=(0, 1))[:2] / (u_dev * n_users)
    return (log_rank[0], metrics)


def solution(mesh):
    return jax.shard_map(
        body,
        mesh=mesh,
        in_specs=(P("users", "items"), P("items", None), P("users"), P("users", None)),
        out_specs=(P("users"), P()),
        check_vma=False,
    )
```

```python
import functools

import jax
import jax.numpy as jnp
from jax import lax
from jax.experimental import pallas as pl
from jax.experimental.pallas import tpu as pltpu
from jax.sharding import PartitionSpec as P

sharpness = 4.0
block_items = 4096
chunk_items = 512
chunk_users = 256
largest = 1e37


def spread_kernel(own, target, history, out, table, sem, *, item_dev):
    for i in range(out.shape[0]):
        pltpu.make_async_copy(own, out.at[i], sem).start()
    shard = lax.axis_index("items")
    goal = target[...]
    past = history[pl.ds(shard, 1), :]
    local = goal - shard * item_dev
    seen = jnp.any(history[...] == goal, axis=0, keepdims=True)
    inside = (local >= 0) & (local < item_dev)
    table[0:1, :] = (goal & (item_dev - 1)) >> 3
    table[1:2, :] = (past & (item_dev - 1)) >> 3
    table[2:3, :] = goal & 7
    table[3:4, :] = past & 7
    table[4:5, :] = inside.astype(jnp.int32)
    table[5:6, :] = seen.astype(jnp.int32)
    owned = inside.astype(jnp.int32)
    for shift in (1, 2, 4):
        owned = jnp.maximum(owned, pltpu.roll(owned, shift, 1))
    table[6:7, :] = owned
    table[7:8, :] = jnp.zeros_like(owned)
    pltpu.make_async_copy(out, out, sem).wait()


def gather_kernel(scalars, table, tiles, trow, hrow, notes, head, tbuf, hbuf, tsem, hsem, lsem):
    u_dev = table.shape[1]
    lead = pltpu.make_async_copy(tiles.at[pl.ds(0, head.shape[0])], head, lsem)

    def start(row, buf, sem):
        def some(i, _):
            for k in range(16):
                u = i * 16 + k
                pltpu.make_async_copy(tiles.at[scalars[row, u]], buf.at[u], sem).start(priority=k % 2)
            return 0

        lax.fori_loop(0, u_dev // 16, some, 0)

    start(1, hbuf, hsem)
    start(0, tbuf, tsem)
    lead.start()
    notes[0:1, :] = table[4:5, :].astype(jnp.float32)
    notes[1:2, :] = jnp.where(table[5:6, :] > 0, 0.0, 0.5)
    n = 128
    at = lax.broadcasted_iota(jnp.int32, (n * 8, n), 0)
    lane = lax.broadcasted_iota(jnp.int32, (1, n), 1) * 8
    for row, buf, sem, out in ((3, hbuf, hsem, hrow), (2, tbuf, tsem, trow)):
        pltpu.make_async_copy(buf, buf, sem).wait()
        for b in range(u_dev // n):
            rows = buf[b * n : (b + 1) * n].reshape(n * 8, buf.shape[2])
            own = lane + table[row : row + 1, b * n : (b + 1) * n]
            pick = jnp.where(at == own, 1.0, 0.0).astype(jnp.bfloat16)
            out[b * n : (b + 1) * n, :] = lax.dot_general(
                pick, rows, (((0,), (0,)), ((), ())), preferred_element_type=jnp.float32
            ).astype(jnp.bfloat16)
    lead.wait()


def own_scores(rows, users):
    n = 128
    own = lax.broadcasted_iota(jnp.int32, (n, n), 0) == lax.broadcasted_iota(jnp.int32, (n, n), 1)
    scores = []
    for b in range(rows.shape[0] // n):
        at = slice(b * n, (b + 1) * n)
        every = jnp.dot(rows[at, :], users[:, at], preferred_element_type=jnp.float32)
        scores.append(jnp.sum(jnp.where(own, every, 0.0), axis=0, keepdims=True))
    return jnp.concatenate(scores, axis=1)


def tscore_kernel(users, trow, notes, out):
    part = jnp.where(notes[0:1, :] > 0.0, own_scores(trow, users), 0.0)
    out[...] = jnp.broadcast_to(part[None], out.shape)


def count_kernel(users, hrow, parts, head, items, out, block, scaled, total, far, tscore, sems):
    u_dev = users.shape[1]
    n_blocks = items.shape[0] // block_items

    def fetch(i):
        at = pl.ds(pl.multiple_of(i * block_items, block_items), block_items)
        return pltpu.make_async_copy(items.at[at, :], block.at[lax.rem(i, 3)], sems.at[lax.rem(i, 3)])

    part = head.shape[0]
    rest = pltpu.make_async_copy(
        items.at[pl.ds(part, block_items - part), :], block.at[0, pl.ds(part, block_items - part), :], sems.at[0]
    )
    rest.start()
    fetch(1).start()
    fetch(2).start()
    block[0, :part, :] = head[...]
    total[...] = jnp.zeros_like(total)
    far[...] = jnp.zeros_like(far)
    ts = jnp.sum(parts[...], axis=0)
    tscore[...] = ts
    scaled[...] = users[...] * jnp.bfloat16(-sharpness)
    hscore = own_scores(hrow, users)
    taken = 1.0 / (1.0 + jnp.exp(jnp.minimum(sharpness * (ts - hscore), 80.0)))

    def step(i, _):
        @pl.when((i > 0) & (i + 2 < n_blocks))
        def _():
            fetch(i + 2).start()

        @pl.when(i == 0)
        def _():
            rest.wait()

        @pl.when(i > 0)
        def _():
            fetch(i).wait()

        slot = lax.rem(i, 3)
        for n in range(u_dev // chunk_users):
            cols = slice(n * chunk_users, (n + 1) * chunk_users)
            w = scaled[:, cols]
            base = jnp.exp(-sharpness * tscore[:, cols])
            acc = total[:, cols]
            top = far[:, cols]
            for c in range(block_items // chunk_items):
                x = jnp.dot(
                    block[slot, c * chunk_items : (c + 1) * chunk_items, :], w, preferred_element_type=jnp.float32
                )
                d = (jnp.exp(x) + base).reshape(chunk_items // 16, 2, 8, chunk_users)
                both = d[:, 0] * d[:, 1]
                acc = acc + jnp.sum((d[:, 0] + d[:, 1]) * (1.0 / both), axis=0)
                top = jnp.maximum(top, jnp.max(both, axis=0))
            total[:, cols] = acc
            far[:, cols] = top
        return 0

    lax.fori_loop(0, n_blocks, step, 0)
    base = jnp.exp(-sharpness * ts)
    count = jnp.sum(total[...], axis=0, keepdims=True) * base
    good = (jnp.max(far[...], axis=0, keepdims=True) < largest) & (jnp.abs(sharpness * ts) < 60.0)
    good = good & (count < largest)
    out[...] = jnp.broadcast_to((count - taken)[None], out.shape)
    bad = jnp.sum(jnp.where(good, 0.0, 1.0))

    @pl.when(bad > 0.0)
    def _():
        total[...] = jnp.zeros_like(total)

        def again(i, _):
            rows = pl.ds(pl.multiple_of(i * 256, 256), 256)
            copy = pltpu.make_async_copy(items.at[rows, :], block.at[0, pl.ds(0, 256), :], sems.at[0])
            copy.start()
            copy.wait()
            for n in range(u_dev // 256):
                cols = slice(n * 256, (n + 1) * 256)
                s = jnp.dot(block[0, :256, :], users[:, cols], preferred_element_type=jnp.float32)
                x = jnp.minimum(sharpness * (tscore[:, cols] - s), 80.0)
                total[:, cols] += jnp.sum((1.0 / (1.0 + jnp.exp(x))).reshape(32, 8, 256), axis=0)
            return 0

        lax.fori_loop(0, items.shape[0] // 256, again, 0)
        exact = jnp.sum(total[...], axis=0, keepdims=True)
        out[...] = jnp.broadcast_to((exact - taken)[None], out.shape)


def metric_kernel(parts, notes, log_rank, sums):
    above = jnp.sum(parts[...], axis=0) - notes[1:2, :]
    rank = 1.0 + above
    log_rank[...] = jnp.log(rank)
    hit = 1.0 / (1.0 + jnp.exp(rank - 10.5))
    gain = hit / (jnp.log(1.0 + rank) * (1.0 / 0.6931471805599453))
    lane = lax.broadcasted_iota(jnp.int32, (1, 128), 1)
    row = jnp.where(lane == 0, jnp.sum(hit), jnp.where(lane == 1, jnp.sum(gain), 0.0))
    sums[...] = jnp.broadcast_to(row[None], sums.shape)


def body(user_emb, item_emb, target, history):
    item_dev, dim = item_emb.shape
    u_dev = user_emb.shape[0]
    n_items = lax.axis_size("items")
    n_users = lax.axis_size("users")
    f32 = jnp.float32
    vmem = pl.BlockSpec(memory_space=pltpu.VMEM)
    hbm = pl.BlockSpec(memory_space=pltpu.HBM)
    smem = pl.BlockSpec(memory_space=pltpu.SMEM)

    small = pltpu.CompilerParams(vmem_limit_bytes=8 * 1024 * 1024)
    columns, table = pl.pallas_call(
        functools.partial(spread_kernel, item_dev=item_dev),
        out_shape=(
            jax.ShapeDtypeStruct((n_items, dim // n_items, u_dev), jnp.bfloat16),
            jax.ShapeDtypeStruct((8, u_dev), jnp.int32),
        ),
        in_specs=[vmem, vmem, vmem],
        out_specs=(hbm, vmem),
        scratch_shapes=[pltpu.SemaphoreType.DMA],
        name="spread",
    )(user_emb.T, target[None], history.T)
    users = lax.all_to_all(columns, "items", split_axis=0, concat_axis=0, tiled=True).reshape(dim, u_dev)

    rows = jax.ShapeDtypeStruct((u_dev, dim), jnp.bfloat16)
    trow, hrow, notes, head = pl.pallas_call(
        gather_kernel,
        out_shape=(
            rows,
            rows,
            jax.ShapeDtypeStruct((2, u_dev), f32),
            jax.ShapeDtypeStruct((block_items // 16, 8, dim), jnp.bfloat16),
        ),
        in_specs=[smem, vmem, hbm],
        out_specs=(vmem, vmem, vmem, vmem),
        scratch_shapes=[
            pltpu.VMEM((u_dev, 8, dim), jnp.bfloat16),
            pltpu.VMEM((u_dev, 8, dim), jnp.bfloat16),
            pltpu.SemaphoreType.DMA,
            pltpu.SemaphoreType.DMA,
            pltpu.SemaphoreType.DMA,
        ],
        compiler_params=pltpu.CompilerParams(vmem_limit_bytes=40 * 1024 * 1024),
        name="gather",
    )(table, table, item_emb.reshape(item_dev // 8, 8, dim))

    spread = jax.ShapeDtypeStruct((n_items, 1, u_dev), f32)
    part_t = pl.pallas_call(
        tscore_kernel,
        out_shape=spread,
        in_specs=[vmem] * 3,
        out_specs=vmem,
        compiler_params=small,
        name="tscore",
    )(users, trow, notes)
    parts_t = lax.all_to_all(part_t, "items", split_axis=0, concat_axis=0, tiled=True)

    local = pl.pallas_call(
        count_kernel,
        out_shape=spread,
        in_specs=[vmem, vmem, vmem, vmem, hbm],
        out_specs=vmem,
        scratch_shapes=[
            pltpu.VMEM((3, block_items, dim), jnp.bfloat16),
            pltpu.VMEM((dim, u_dev), jnp.bfloat16),
            pltpu.VMEM((8, u_dev), f32),
            pltpu.VMEM((8, u_dev), f32),
            pltpu.VMEM((1, u_dev), f32),
            pltpu.SemaphoreType.DMA((3,)),
        ],
        compiler_params=pltpu.CompilerParams(
            vmem_limit_bytes=40 * 1024 * 1024,
        ),
        name="count",
    )(users, hrow, parts_t, head.reshape(block_items // 2, dim), item_emb)

    parts = lax.all_to_all(local, "items", split_axis=0, concat_axis=0, tiled=True)
    log_rank, sums = pl.pallas_call(
        metric_kernel,
        out_shape=(jax.ShapeDtypeStruct((1, u_dev), f32), jax.ShapeDtypeStruct((n_users, 1, 128), f32)),
        in_specs=[vmem, vmem],
        out_specs=(vmem, vmem),
        compiler_params=small,
        name="metric",
    )(parts, notes)
    sums = lax.all_to_all(sums, "users", split_axis=0, concat_axis=0, tiled=True)
    metrics = jnp.sum(sums, axis=(0, 1))[:2] / (u_dev * n_users)
    return (log_rank[0], metrics)


def solution(mesh):
    return jax.shard_map(
        body,
        mesh=mesh,
        in_specs=(P("users", "items"), P("items", None), P("users"), P("users", None)),
        out_specs=(P("users"), P()),
        check_vma=False,
    )
```

```python
import functools

import jax
import jax.numpy as jnp
from jax import lax
from jax.experimental import pallas as pl
from jax.experimental.pallas import tpu as pltpu
from jax.sharding import PartitionSpec as P

sharpness = 4.0
block_items = 4096
chunk_items = 2048
chunk_users = 256
largest = 1e37


def spread_kernel(own, target, history, out, table, rows, sem, tsem, *, item_dev):
    for i in range(out.shape[0]):
        pltpu.make_async_copy(own, out.at[i], sem).start()
    shard = lax.axis_index("items")
    goal = target[...]
    past = history[pl.ds(shard, 1), :]
    local = goal - shard * item_dev
    seen = jnp.any(history[...] == goal, axis=0, keepdims=True)
    inside = (local >= 0) & (local < item_dev)
    rows[0:1, :] = (goal & (item_dev - 1)) >> 3
    rows[1:2, :] = goal & 7
    rows[2:3, :] = inside.astype(jnp.int32)
    rows[3:4, :] = seen.astype(jnp.int32)
    rows[4:5, :] = (past & (item_dev - 1)) >> 3
    rows[5:6, :] = past & 7
    rows[6:8, :] = jnp.zeros_like(rows[6:8, :])
    copy = pltpu.make_async_copy(rows, table, tsem)
    copy.start()
    copy.wait()
    pltpu.make_async_copy(out, out, sem).wait()


def start_rows(scalars, tiles, buf, sem):
    def some(i, _):
        for k in range(16):
            u = i * 16 + k
            pltpu.make_async_copy(tiles.at[scalars[0, u]], buf.at[u], sem).start(priority=k % 2)
        return 0

    lax.fori_loop(0, buf.shape[0] // 16, some, 0)


def pick_rows(table, buf, sem, out):
    pltpu.make_async_copy(buf, buf, sem).wait()
    n = 128
    at = lax.broadcasted_iota(jnp.int32, (n * 8, n), 0)
    lane = lax.broadcasted_iota(jnp.int32, (1, n), 1) * 8
    for b in range(buf.shape[0] // n):
        rows = buf[b * n : (b + 1) * n].reshape(n * 8, buf.shape[2])
        own = lane + table[1:2, b * n : (b + 1) * n]
        pick = jnp.where(at == own, 1.0, 0.0).astype(jnp.bfloat16)
        out[b * n : (b + 1) * n, :] = lax.dot_general(
            pick, rows, (((0,), (0,)), ((), ())), preferred_element_type=jnp.float32
        ).astype(jnp.bfloat16)


def target_kernel(scalars, table, tiles, trow, notes, past, buf, sem):
    start_rows(scalars, tiles, buf, sem)
    notes[0:1, :] = table[2:3, :].astype(jnp.float32)
    notes[1:2, :] = jnp.where(table[3:4, :] > 0, 0.0, 0.5)
    past[...] = table[4:6, :]
    pick_rows(table, buf, sem, trow)


def history_kernel(scalars, table, token, tiles, hrow, head, buf, sem, lsem):
    start_rows(scalars, tiles, buf, sem)
    lead = pltpu.make_async_copy(tiles.at[pl.ds(0, head.shape[0])], head, lsem)
    lead.start()
    pick_rows(table, buf, sem, hrow)
    lead.wait()


def own_scores(rows, users):
    n = 128
    own = lax.broadcasted_iota(jnp.int32, (n, n), 0) == lax.broadcasted_iota(jnp.int32, (n, n), 1)
    scores = []
    for b in range(rows.shape[0] // n):
        at = slice(b * n, (b + 1) * n)
        every = jnp.dot(rows[at, :], users[:, at], preferred_element_type=jnp.float32)
        scores.append(jnp.sum(jnp.where(own, every, 0.0), axis=0, keepdims=True))
    return jnp.concatenate(scores, axis=1)


def tscore_kernel(users, trow, notes, out, token):
    token[...] = jnp.zeros_like(token)
    part = jnp.where(notes[0:1, :] > 0.0, own_scores(trow, users), 0.0)
    out[...] = jnp.broadcast_to(part[None], out.shape)


def count_kernel(users, hrow, parts, head, items, out, block, scaled, total, far, tscore, sems):
    u_dev = users.shape[1]
    n_blocks = items.shape[0] // block_items

    def fetch(i):
        at = pl.ds(pl.multiple_of(i * block_items, block_items), block_items)
        return pltpu.make_async_copy(items.at[at, :], block.at[lax.rem(i, 3)], sems.at[lax.rem(i, 3)])

    fetch(1).start()
    fetch(2).start()
    block[0] = head[...]
    total[...] = jnp.zeros_like(total)
    far[...] = jnp.zeros_like(far)
    ts = jnp.sum(parts[...], axis=0)
    tscore[...] = ts
    scaled[...] = users[...] * jnp.bfloat16(-sharpness)
    hscore = own_scores(hrow, users)
    taken = 1.0 / (1.0 + jnp.exp(jnp.minimum(sharpness * (ts - hscore), 80.0)))

    def step(i, _):
        @pl.when((i > 0) & (i + 2 < n_blocks))
        def _():
            fetch(i + 2).start()

        @pl.when(i > 0)
        def _():
            fetch(i).wait()

        slot = lax.rem(i, 3)
        for n in range(u_dev // chunk_users):
            cols = slice(n * chunk_users, (n + 1) * chunk_users)
            w = scaled[:, cols]
            base = jnp.exp(-sharpness * tscore[:, cols])
            acc = total[:, cols]
            top = far[:, cols]
            for c in range(block_items // chunk_items):
                x = jnp.dot(
                    block[slot, c * chunk_items : (c + 1) * chunk_items, :], w, preferred_element_type=jnp.float32
                )
                d = (jnp.exp(x) + base).reshape(chunk_items // 16, 2, 8, chunk_users)
                both = d[:, 0] * d[:, 1]
                acc = acc + jnp.sum((d[:, 0] + d[:, 1]) * (1.0 / both), axis=0)
                top = jnp.maximum(top, jnp.max(both, axis=0))
            total[:, cols] = acc
            far[:, cols] = top
        return 0

    lax.fori_loop(0, n_blocks, step, 0)
    base = jnp.exp(-sharpness * ts)
    count = jnp.sum(total[...], axis=0, keepdims=True) * base
    good = (jnp.max(far[...], axis=0, keepdims=True) < largest) & (jnp.abs(sharpness * ts) < 60.0)
    good = good & (count < largest)
    out[...] = jnp.broadcast_to((count - taken)[None], out.shape)
    bad = jnp.sum(jnp.where(good, 0.0, 1.0))

    @pl.when(bad > 0.0)
    def _():
        total[...] = jnp.zeros_like(total)

        def again(i, _):
            rows = pl.ds(pl.multiple_of(i * 256, 256), 256)
            copy = pltpu.make_async_copy(items.at[rows, :], block.at[0, pl.ds(0, 256), :], sems.at[0])
            copy.start()
            copy.wait()
            for n in range(u_dev // 256):
                cols = slice(n * 256, (n + 1) * 256)
                s = jnp.dot(block[0, :256, :], users[:, cols], preferred_element_type=jnp.float32)
                x = jnp.minimum(sharpness * (tscore[:, cols] - s), 80.0)
                total[:, cols] += jnp.sum((1.0 / (1.0 + jnp.exp(x))).reshape(32, 8, 256), axis=0)
            return 0

        lax.fori_loop(0, items.shape[0] // 256, again, 0)
        exact = jnp.sum(total[...], axis=0, keepdims=True)
        out[...] = jnp.broadcast_to((exact - taken)[None], out.shape)


def metric_kernel(parts, notes, log_rank, sums):
    above = jnp.sum(parts[...], axis=0) - notes[1:2, :]
    rank = 1.0 + above
    log_rank[...] = jnp.log(rank)
    hit = 1.0 / (1.0 + jnp.exp(rank - 10.5))
    gain = hit / (jnp.log(1.0 + rank) * (1.0 / 0.6931471805599453))
    lane = lax.broadcasted_iota(jnp.int32, (1, 128), 1)
    row = jnp.where(lane == 0, jnp.sum(hit), jnp.where(lane == 1, jnp.sum(gain), 0.0))
    sums[...] = jnp.broadcast_to(row[None], sums.shape)


def body(user_emb, item_emb, target, history):
    item_dev, dim = item_emb.shape
    u_dev = user_emb.shape[0]
    n_items = lax.axis_size("items")
    n_users = lax.axis_size("users")
    f32 = jnp.float32
    vmem = pl.BlockSpec(memory_space=pltpu.VMEM)
    hbm = pl.BlockSpec(memory_space=pltpu.HBM)
    smem = pl.BlockSpec(memory_space=pltpu.SMEM)

    small = pltpu.CompilerParams(vmem_limit_bytes=8 * 1024 * 1024)
    columns, table = pl.pallas_call(
        functools.partial(spread_kernel, item_dev=item_dev),
        out_shape=(
            jax.ShapeDtypeStruct((n_items, dim // n_items, u_dev), jnp.bfloat16),
            jax.ShapeDtypeStruct((8, u_dev), jnp.int32),
        ),
        in_specs=[vmem, vmem, vmem],
        out_specs=(hbm, hbm),
        scratch_shapes=[pltpu.VMEM((8, u_dev), jnp.int32), pltpu.SemaphoreType.DMA, pltpu.SemaphoreType.DMA],
        name="spread",
    )(user_emb.T, target[None], history.T)
    users = lax.all_to_all(columns, "items", split_axis=0, concat_axis=0, tiled=True).reshape(dim, u_dev)

    tiles = item_emb.reshape(item_dev // 8, 8, dim)
    rows = jax.ShapeDtypeStruct((u_dev, dim), jnp.bfloat16)
    fetched = pltpu.VMEM((u_dev, 8, dim), jnp.bfloat16)
    trow, notes, past = pl.pallas_call(
        target_kernel,
        out_shape=(rows, jax.ShapeDtypeStruct((2, u_dev), f32), jax.ShapeDtypeStruct((2, u_dev), jnp.int32)),
        in_specs=[smem, vmem, hbm],
        out_specs=(vmem, vmem, vmem),
        scratch_shapes=[fetched, pltpu.SemaphoreType.DMA],
        compiler_params=pltpu.CompilerParams(vmem_limit_bytes=44 * 1024 * 1024),
        name="target",
    )(table, table, tiles)

    spread = jax.ShapeDtypeStruct((n_items, 1, u_dev), f32)
    part_t, token = pl.pallas_call(
        tscore_kernel,
        out_shape=(spread, jax.ShapeDtypeStruct((8, 128), f32)),
        in_specs=[vmem] * 3,
        out_specs=(vmem, vmem),
        compiler_params=small,
        name="tscore",
    )(users, trow, notes)
    parts_t = lax.all_to_all(part_t, "items", split_axis=0, concat_axis=0, tiled=True)
    hrow, head = pl.pallas_call(
        history_kernel,
        out_shape=(rows, jax.ShapeDtypeStruct((block_items // 8, 8, dim), jnp.bfloat16)),
        in_specs=[smem, vmem, vmem, hbm],
        out_specs=(vmem, vmem),
        scratch_shapes=[fetched, pltpu.SemaphoreType.DMA, pltpu.SemaphoreType.DMA],
        compiler_params=pltpu.CompilerParams(vmem_limit_bytes=44 * 1024 * 1024),
        name="history",
    )(past, past, token, tiles)

    local = pl.pallas_call(
        count_kernel,
        out_shape=spread,
        in_specs=[vmem, vmem, vmem, vmem, hbm],
        out_specs=vmem,
        scratch_shapes=[
            pltpu.VMEM((3, block_items, dim), jnp.bfloat16),
            pltpu.VMEM((dim, u_dev), jnp.bfloat16),
            pltpu.VMEM((8, u_dev), f32),
            pltpu.VMEM((8, u_dev), f32),
            pltpu.VMEM((1, u_dev), f32),
            pltpu.SemaphoreType.DMA((3,)),
        ],
        compiler_params=pltpu.CompilerParams(
            vmem_limit_bytes=40 * 1024 * 1024,
        ),
        name="count",
    )(users, hrow, parts_t, head.reshape(block_items, dim), item_emb)

    parts = lax.all_to_all(local, "items", split_axis=0, concat_axis=0, tiled=True)
    log_rank, sums = pl.pallas_call(
        metric_kernel,
        out_shape=(jax.ShapeDtypeStruct((1, u_dev), f32), jax.ShapeDtypeStruct((n_users, 1, 128), f32)),
        in_specs=[vmem, vmem],
        out_specs=(vmem, vmem),
        compiler_params=small,
        name="metric",
    )(parts, notes)
    sums = lax.all_to_all(sums, "users", split_axis=0, concat_axis=0, tiled=True)
    metrics = jnp.sum(sums, axis=(0, 1))[:2] / (u_dev * n_users)
    return (log_rank[0], metrics)


def solution(mesh):
    return jax.shard_map(
        body,
        mesh=mesh,
        in_specs=(P("users", "items"), P("items", None), P("users"), P("users", None)),
        out_specs=(P("users"), P()),
        check_vma=False,
    )
```

```python
import functools

import jax
import jax.numpy as jnp
from jax import lax
from jax.experimental import pallas as pl
from jax.experimental.pallas import tpu as pltpu
from jax.sharding import PartitionSpec as P

sharpness = 4.0
block_items = 4096
chunk_items = 2048
chunk_users = 256
early_users = 384
largest = 1e37


def spread_kernel(own, target, history, out, table, rows, sem, tsem, *, item_dev):
    for i in range(out.shape[0]):
        pltpu.make_async_copy(own, out.at[i], sem).start()
    shard = lax.axis_index("items")
    goal = target[...]
    past = history[pl.ds(shard, 1), :]
    local = goal - shard * item_dev
    seen = jnp.any(history[...] == goal, axis=0, keepdims=True)
    inside = (local >= 0) & (local < item_dev)
    rows[0:1, :] = (goal & (item_dev - 1)) >> 3
    rows[1:2, :] = goal & 7
    rows[2:3, :] = inside.astype(jnp.int32)
    rows[3:4, :] = seen.astype(jnp.int32)
    rows[4:5, :] = (past & (item_dev - 1)) >> 3
    rows[5:6, :] = past & 7
    rows[6:8, :] = jnp.zeros_like(rows[6:8, :])
    copy = pltpu.make_async_copy(rows, table, tsem)
    copy.start()
    copy.wait()
    pltpu.make_async_copy(out, out, sem).wait()


def start_rows(scalars, row, first, tiles, buf, sem):
    def some(i, _):
        for k in range(16):
            u = i * 16 + k
            pltpu.make_async_copy(tiles.at[scalars[row, first + u]], buf.at[u], sem).start(priority=k % 2)
        return 0

    lax.fori_loop(0, buf.shape[0] // 16, some, 0)


def pick_rows(table, row, first, buf, sem, out):
    pltpu.make_async_copy(buf, buf, sem).wait()
    n = 128
    at = lax.broadcasted_iota(jnp.int32, (n * 8, n), 0)
    lane = lax.broadcasted_iota(jnp.int32, (1, n), 1) * 8
    for b in range(buf.shape[0] // n):
        rows = buf[b * n : (b + 1) * n].reshape(n * 8, buf.shape[2])
        own = lane + table[row : row + 1, first + b * n : first + (b + 1) * n]
        pick = jnp.where(at == own, 1.0, 0.0).astype(jnp.bfloat16)
        out[b * n : (b + 1) * n, :] = lax.dot_general(
            pick, rows, (((0,), (0,)), ((), ())), preferred_element_type=jnp.float32
        ).astype(jnp.bfloat16)


def target_kernel(scalars, table, tiles, trow, hrow, notes, past, buf, hbuf, sem, hsem):
    start_rows(scalars, 0, 0, tiles, buf, sem)
    start_rows(scalars, 4, 0, tiles, hbuf, hsem)
    notes[0:1, :] = table[2:3, :].astype(jnp.float32)
    notes[1:2, :] = jnp.where(table[3:4, :] > 0, 0.0, 0.5)
    past[...] = table[4:6, :]
    pick_rows(table, 1, 0, buf, sem, trow)
    pick_rows(table, 5, 0, hbuf, hsem, hrow)


def history_kernel(scalars, table, token, tiles, hrow, head, buf, sem, lsem):
    first = table.shape[1] - buf.shape[0]
    start_rows(scalars, 0, first, tiles, buf, sem)
    lead = pltpu.make_async_copy(tiles.at[pl.ds(0, head.shape[0])], head, lsem)
    lead.start()
    pick_rows(table, 1, first, buf, sem, hrow)
    lead.wait()


def own_scores(rows, users, first=0):
    n = 128
    own = lax.broadcasted_iota(jnp.int32, (n, n), 0) == lax.broadcasted_iota(jnp.int32, (n, n), 1)
    scores = []
    for b in range(rows.shape[0] // n):
        every = jnp.dot(
            rows[b * n : (b + 1) * n, :],
            users[:, first + b * n : first + (b + 1) * n],
            preferred_element_type=jnp.float32,
        )
        scores.append(jnp.sum(jnp.where(own, every, 0.0), axis=0, keepdims=True))
    return jnp.concatenate(scores, axis=1)


def tscore_kernel(users, trow, notes, out, token):
    token[...] = jnp.zeros_like(token)
    part = jnp.where(notes[0:1, :] > 0.0, own_scores(trow, users), 0.0)
    out[...] = jnp.broadcast_to(part[None], out.shape)


def count_kernel(users, hrow_a, hrow_b, parts, head, items, out, block, scaled, total, far, tscore, sems):
    u_dev = users.shape[1]
    n_blocks = items.shape[0] // block_items

    def fetch(i):
        at = pl.ds(pl.multiple_of(i * block_items, block_items), block_items)
        return pltpu.make_async_copy(items.at[at, :], block.at[lax.rem(i, 3)], sems.at[lax.rem(i, 3)])

    fetch(1).start()
    fetch(2).start()
    block[0] = head[...]
    total[...] = jnp.zeros_like(total)
    far[...] = jnp.zeros_like(far)
    ts = jnp.sum(parts[...], axis=0)
    tscore[...] = ts
    scaled[...] = users[...] * jnp.bfloat16(-sharpness)
    early = hrow_a.shape[0]
    hscore = jnp.concatenate([own_scores(hrow_a, users), own_scores(hrow_b, users, early)], axis=1)
    taken = 1.0 / (1.0 + jnp.exp(jnp.minimum(sharpness * (ts - hscore), 80.0)))

    def step(i, _):
        @pl.when((i > 0) & (i + 2 < n_blocks))
        def _():
            fetch(i + 2).start()

        @pl.when(i > 0)
        def _():
            fetch(i).wait()

        slot = lax.rem(i, 3)
        for n in range(u_dev // chunk_users):
            cols = slice(n * chunk_users, (n + 1) * chunk_users)
            w = scaled[:, cols]
            base = jnp.exp(-sharpness * tscore[:, cols])
            acc = total[:, cols]
            top = far[:, cols]
            for c in range(block_items // chunk_items):
                x = jnp.dot(
                    block[slot, c * chunk_items : (c + 1) * chunk_items, :], w, preferred_element_type=jnp.float32
                )
                d = (jnp.exp(x) + base).reshape(chunk_items // 16, 2, 8, chunk_users)
                both = d[:, 0] * d[:, 1]
                acc = acc + jnp.sum((d[:, 0] + d[:, 1]) * (1.0 / both), axis=0)
                top = jnp.maximum(top, jnp.max(both, axis=0))
            total[:, cols] = acc
            far[:, cols] = top
        return 0

    lax.fori_loop(0, n_blocks, step, 0)
    base = jnp.exp(-sharpness * ts)
    count = jnp.sum(total[...], axis=0, keepdims=True) * base
    good = (jnp.max(far[...], axis=0, keepdims=True) < largest) & (jnp.abs(sharpness * ts) < 60.0)
    good = good & (count < largest)
    out[...] = jnp.broadcast_to((count - taken)[None], out.shape)
    bad = jnp.sum(jnp.where(good, 0.0, 1.0))

    @pl.when(bad > 0.0)
    def _():
        total[...] = jnp.zeros_like(total)

        def again(i, _):
            rows = pl.ds(pl.multiple_of(i * 256, 256), 256)
            copy = pltpu.make_async_copy(items.at[rows, :], block.at[0, pl.ds(0, 256), :], sems.at[0])
            copy.start()
            copy.wait()
            for n in range(u_dev // 256):
                cols = slice(n * 256, (n + 1) * 256)
                s = jnp.dot(block[0, :256, :], users[:, cols], preferred_element_type=jnp.float32)
                x = jnp.minimum(sharpness * (tscore[:, cols] - s), 80.0)
                total[:, cols] += jnp.sum((1.0 / (1.0 + jnp.exp(x))).reshape(32, 8, 256), axis=0)
            return 0

        lax.fori_loop(0, items.shape[0] // 256, again, 0)
        exact = jnp.sum(total[...], axis=0, keepdims=True)
        out[...] = jnp.broadcast_to((exact - taken)[None], out.shape)


def metric_kernel(parts, notes, log_rank, sums):
    above = jnp.sum(parts[...], axis=0) - notes[1:2, :]
    rank = 1.0 + above
    log_rank[...] = jnp.log(rank)
    hit = 1.0 / (1.0 + jnp.exp(rank - 10.5))
    gain = hit / (jnp.log(1.0 + rank) * (1.0 / 0.6931471805599453))
    lane = lax.broadcasted_iota(jnp.int32, (1, 128), 1)
    row = jnp.where(lane == 0, jnp.sum(hit), jnp.where(lane == 1, jnp.sum(gain), 0.0))
    sums[...] = jnp.broadcast_to(row[None], sums.shape)


def body(user_emb, item_emb, target, history):
    item_dev, dim = item_emb.shape
    u_dev = user_emb.shape[0]
    n_items = lax.axis_size("items")
    n_users = lax.axis_size("users")
    f32 = jnp.float32
    vmem = pl.BlockSpec(memory_space=pltpu.VMEM)
    hbm = pl.BlockSpec(memory_space=pltpu.HBM)
    smem = pl.BlockSpec(memory_space=pltpu.SMEM)

    small = pltpu.CompilerParams(vmem_limit_bytes=8 * 1024 * 1024)
    columns, table = pl.pallas_call(
        functools.partial(spread_kernel, item_dev=item_dev),
        out_shape=(
            jax.ShapeDtypeStruct((n_items, dim // n_items, u_dev), jnp.bfloat16),
            jax.ShapeDtypeStruct((8, u_dev), jnp.int32),
        ),
        in_specs=[vmem, vmem, vmem],
        out_specs=(hbm, hbm),
        scratch_shapes=[pltpu.VMEM((8, u_dev), jnp.int32), pltpu.SemaphoreType.DMA, pltpu.SemaphoreType.DMA],
        name="spread",
    )(user_emb.T, target[None], history.T)
    users = lax.all_to_all(columns, "items", split_axis=0, concat_axis=0, tiled=True).reshape(dim, u_dev)

    tiles = item_emb.reshape(item_dev // 8, 8, dim)
    rows = lambda n: jax.ShapeDtypeStruct((n, dim), jnp.bfloat16)
    fetched = lambda n: pltpu.VMEM((n, 8, dim), jnp.bfloat16)
    trow, hrow_a, notes, past = pl.pallas_call(
        target_kernel,
        out_shape=(
            rows(u_dev),
            rows(early_users),
            jax.ShapeDtypeStruct((2, u_dev), f32),
            jax.ShapeDtypeStruct((2, u_dev), jnp.int32),
        ),
        in_specs=[smem, vmem, hbm],
        out_specs=(vmem, vmem, vmem, vmem),
        scratch_shapes=[
            fetched(u_dev),
            fetched(early_users),
            pltpu.SemaphoreType.DMA,
            pltpu.SemaphoreType.DMA,
        ],
        compiler_params=pltpu.CompilerParams(vmem_limit_bytes=44 * 1024 * 1024),
        name="target",
    )(table, table, tiles)

    spread = jax.ShapeDtypeStruct((n_items, 1, u_dev), f32)
    part_t, token = pl.pallas_call(
        tscore_kernel,
        out_shape=(spread, jax.ShapeDtypeStruct((8, 128), f32)),
        in_specs=[vmem] * 3,
        out_specs=(vmem, vmem),
        compiler_params=small,
        name="tscore",
    )(users, trow, notes)
    parts_t = lax.all_to_all(part_t, "items", split_axis=0, concat_axis=0, tiled=True)
    hrow_b, head = pl.pallas_call(
        history_kernel,
        out_shape=(rows(u_dev - early_users), jax.ShapeDtypeStruct((block_items // 8, 8, dim), jnp.bfloat16)),
        in_specs=[smem, vmem, vmem, hbm],
        out_specs=(vmem, vmem),
        scratch_shapes=[fetched(u_dev - early_users), pltpu.SemaphoreType.DMA, pltpu.SemaphoreType.DMA],
        compiler_params=pltpu.CompilerParams(vmem_limit_bytes=44 * 1024 * 1024),
        name="history",
    )(past, past, token, tiles)

    local = pl.pallas_call(
        count_kernel,
        out_shape=spread,
        in_specs=[vmem, vmem, vmem, vmem, vmem, hbm],
        out_specs=vmem,
        scratch_shapes=[
            pltpu.VMEM((3, block_items, dim), jnp.bfloat16),
            pltpu.VMEM((dim, u_dev), jnp.bfloat16),
            pltpu.VMEM((8, u_dev), f32),
            pltpu.VMEM((8, u_dev), f32),
            pltpu.VMEM((1, u_dev), f32),
            pltpu.SemaphoreType.DMA((3,)),
        ],
        compiler_params=pltpu.CompilerParams(
            vmem_limit_bytes=40 * 1024 * 1024,
        ),
        name="count",
    )(users, hrow_a, hrow_b, parts_t, head.reshape(block_items, dim), item_emb)

    parts = lax.all_to_all(local, "items", split_axis=0, concat_axis=0, tiled=True)
    log_rank, sums = pl.pallas_call(
        metric_kernel,
        out_shape=(jax.ShapeDtypeStruct((1, u_dev), f32), jax.ShapeDtypeStruct((n_users, 1, 128), f32)),
        in_specs=[vmem, vmem],
        out_specs=(vmem, vmem),
        compiler_params=small,
        name="metric",
    )(parts, notes)
    sums = lax.all_to_all(sums, "users", split_axis=0, concat_axis=0, tiled=True)
    metrics = jnp.sum(sums, axis=(0, 1))[:2] / (u_dev * n_users)
    return (log_rank[0], metrics)


def solution(mesh):
    return jax.shard_map(
        body,
        mesh=mesh,
        in_specs=(P("users", "items"), P("items", None), P("users"), P("users", None)),
        out_specs=(P("users"), P()),
        check_vma=False,
    )
```

```python
import functools

import jax
import jax.numpy as jnp
from jax import lax
from jax.experimental import pallas as pl
from jax.experimental.pallas import tpu as pltpu
from jax.sharding import PartitionSpec as P

sharpness = 4.0
block_items = 4096
chunk_items = 2048
chunk_users = 256
early_users = 512
largest = 1e37


def spread_kernel(own, target, history, out, table, rows, sem, tsem, *, item_dev):
    for i in range(out.shape[0]):
        pltpu.make_async_copy(own, out.at[i], sem).start()
    shard = lax.axis_index("items")
    goal = target[...]
    past = history[pl.ds(shard, 1), :]
    local = goal - shard * item_dev
    seen = jnp.any(history[...] == goal, axis=0, keepdims=True)
    inside = (local >= 0) & (local < item_dev)
    rows[0:1, :] = (goal & (item_dev - 1)) >> 3
    rows[1:2, :] = goal & 7
    rows[2:3, :] = inside.astype(jnp.int32)
    rows[3:4, :] = seen.astype(jnp.int32)
    rows[4:5, :] = (past & (item_dev - 1)) >> 3
    rows[5:6, :] = past & 7
    rows[6:8, :] = jnp.zeros_like(rows[6:8, :])
    copy = pltpu.make_async_copy(rows, table, tsem)
    copy.start()
    copy.wait()
    pltpu.make_async_copy(out, out, sem).wait()


def start_rows(scalars, row, first, tiles, buf, sem):
    def some(i, _):
        for k in range(16):
            u = i * 16 + k
            pltpu.make_async_copy(tiles.at[scalars[row, first + u]], buf.at[u], sem).start(priority=k % 2)
        return 0

    lax.fori_loop(0, buf.shape[0] // 16, some, 0)


def pick_rows(table, row, first, buf, sem, out):
    pltpu.make_async_copy(buf, buf, sem).wait()
    n = 128
    at = lax.broadcasted_iota(jnp.int32, (n * 8, n), 0)
    lane = lax.broadcasted_iota(jnp.int32, (1, n), 1) * 8
    for b in range(buf.shape[0] // n):
        rows = buf[b * n : (b + 1) * n].reshape(n * 8, buf.shape[2])
        own = lane + table[row : row + 1, first + b * n : first + (b + 1) * n]
        pick = jnp.where(at == own, 1.0, 0.0).astype(jnp.bfloat16)
        out[b * n : (b + 1) * n, :] = lax.dot_general(
            pick, rows, (((0,), (0,)), ((), ())), preferred_element_type=jnp.float32
        ).astype(jnp.bfloat16)


def target_kernel(scalars, table, tiles, trow, hrow, notes, past, buf, hbuf, sem, hsem):
    start_rows(scalars, 0, 0, tiles, buf, sem)
    start_rows(scalars, 4, 0, tiles, hbuf, hsem)
    notes[0:1, :] = table[2:3, :].astype(jnp.float32)
    notes[1:2, :] = jnp.where(table[3:4, :] > 0, 0.0, 0.5)
    past[...] = table[4:6, :]
    pick_rows(table, 1, 0, buf, sem, trow)
    pick_rows(table, 5, 0, hbuf, hsem, hrow)


def history_kernel(scalars, table, token, tiles, hrow, head, buf, sem, lsem):
    first = table.shape[1] - buf.shape[0]
    start_rows(scalars, 0, first, tiles, buf, sem)
    lead = pltpu.make_async_copy(tiles.at[pl.ds(0, head.shape[0])], head, lsem)
    lead.start()
    pick_rows(table, 1, first, buf, sem, hrow)
    lead.wait()


def own_scores(rows, users, first=0):
    n = 128
    own = lax.broadcasted_iota(jnp.int32, (n, n), 0) == lax.broadcasted_iota(jnp.int32, (n, n), 1)
    scores = []
    for b in range(rows.shape[0] // n):
        every = jnp.dot(
            rows[b * n : (b + 1) * n, :],
            users[:, first + b * n : first + (b + 1) * n],
            preferred_element_type=jnp.float32,
        )
        scores.append(jnp.sum(jnp.where(own, every, 0.0), axis=0, keepdims=True))
    return jnp.concatenate(scores, axis=1)


def tscore_kernel(users, trow, notes, out, token):
    token[...] = jnp.zeros_like(token)
    part = jnp.where(notes[0:1, :] > 0.0, own_scores(trow, users), 0.0)
    out[...] = jnp.broadcast_to(part[None], out.shape)


def count_kernel(users, hrow_a, hrow_b, parts, head, items, out, block, scaled, total, far, tscore, sems):
    u_dev = users.shape[1]
    n_blocks = items.shape[0] // block_items

    def fetch(i):
        at = pl.ds(pl.multiple_of(i * block_items, block_items), block_items)
        return pltpu.make_async_copy(items.at[at, :], block.at[lax.rem(i, 3)], sems.at[lax.rem(i, 3)])

    fetch(1).start()
    fetch(2).start()
    block[0] = head[...]
    total[...] = jnp.zeros_like(total)
    far[...] = jnp.zeros_like(far)
    ts = jnp.sum(parts[...], axis=0)
    tscore[...] = ts
    scaled[...] = users[...] * jnp.bfloat16(-sharpness)
    early = hrow_a.shape[0]
    hscore = jnp.concatenate([own_scores(hrow_a, users), own_scores(hrow_b, users, early)], axis=1)
    taken = 1.0 / (1.0 + jnp.exp(jnp.minimum(sharpness * (ts - hscore), 80.0)))

    def step(i, _):
        @pl.when((i > 0) & (i + 2 < n_blocks))
        def _():
            fetch(i + 2).start()

        @pl.when(i > 0)
        def _():
            fetch(i).wait()

        slot = lax.rem(i, 3)
        for n in range(u_dev // chunk_users):
            cols = slice(n * chunk_users, (n + 1) * chunk_users)
            w = scaled[:, cols]
            base = jnp.exp(-sharpness * tscore[:, cols])
            acc = total[:, cols]
            top = far[:, cols]
            for c in range(block_items // chunk_items):
                x = jnp.dot(
                    block[slot, c * chunk_items : (c + 1) * chunk_items, :], w, preferred_element_type=jnp.float32
                )
                d = (jnp.exp(x) + base).reshape(chunk_items // 16, 2, 8, chunk_users)
                both = d[:, 0] * d[:, 1]
                acc = acc + jnp.sum((d[:, 0] + d[:, 1]) * (1.0 / both), axis=0)
                top = jnp.maximum(top, jnp.max(both, axis=0))
            total[:, cols] = acc
            far[:, cols] = top
        return 0

    lax.fori_loop(0, n_blocks, step, 0)
    base = jnp.exp(-sharpness * ts)
    count = jnp.sum(total[...], axis=0, keepdims=True) * base
    good = (jnp.max(far[...], axis=0, keepdims=True) < largest) & (jnp.abs(sharpness * ts) < 60.0)
    good = good & (count < largest)
    out[...] = jnp.broadcast_to((count - taken)[None], out.shape)
    bad = jnp.sum(jnp.where(good, 0.0, 1.0))

    @pl.when(bad > 0.0)
    def _():
        total[...] = jnp.zeros_like(total)

        def again(i, _):
            rows = pl.ds(pl.multiple_of(i * 256, 256), 256)
            copy = pltpu.make_async_copy(items.at[rows, :], block.at[0, pl.ds(0, 256), :], sems.at[0])
            copy.start()
            copy.wait()
            for n in range(u_dev // 256):
                cols = slice(n * 256, (n + 1) * 256)
                s = jnp.dot(block[0, :256, :], users[:, cols], preferred_element_type=jnp.float32)
                x = jnp.minimum(sharpness * (tscore[:, cols] - s), 80.0)
                total[:, cols] += jnp.sum((1.0 / (1.0 + jnp.exp(x))).reshape(32, 8, 256), axis=0)
            return 0

        lax.fori_loop(0, items.shape[0] // 256, again, 0)
        exact = jnp.sum(total[...], axis=0, keepdims=True)
        out[...] = jnp.broadcast_to((exact - taken)[None], out.shape)


def metric_kernel(parts, notes, log_rank, sums):
    above = jnp.sum(parts[...], axis=0) - notes[1:2, :]
    rank = 1.0 + above
    log_rank[...] = jnp.log(rank)
    hit = 1.0 / (1.0 + jnp.exp(rank - 10.5))
    gain = hit / (jnp.log(1.0 + rank) * (1.0 / 0.6931471805599453))
    lane = lax.broadcasted_iota(jnp.int32, (1, 128), 1)
    row = jnp.where(lane == 0, jnp.sum(hit), jnp.where(lane == 1, jnp.sum(gain), 0.0))
    sums[...] = jnp.broadcast_to(row[None], sums.shape)


def body(user_emb, item_emb, target, history):
    item_dev, dim = item_emb.shape
    u_dev = user_emb.shape[0]
    n_items = lax.axis_size("items")
    n_users = lax.axis_size("users")
    f32 = jnp.float32
    vmem = pl.BlockSpec(memory_space=pltpu.VMEM)
    hbm = pl.BlockSpec(memory_space=pltpu.HBM)
    smem = pl.BlockSpec(memory_space=pltpu.SMEM)

    small = pltpu.CompilerParams(vmem_limit_bytes=8 * 1024 * 1024)
    columns, table = pl.pallas_call(
        functools.partial(spread_kernel, item_dev=item_dev),
        out_shape=(
            jax.ShapeDtypeStruct((n_items, dim // n_items, u_dev), jnp.bfloat16),
            jax.ShapeDtypeStruct((8, u_dev), jnp.int32),
        ),
        in_specs=[vmem, vmem, vmem],
        out_specs=(hbm, hbm),
        scratch_shapes=[pltpu.VMEM((8, u_dev), jnp.int32), pltpu.SemaphoreType.DMA, pltpu.SemaphoreType.DMA],
        name="spread",
    )(user_emb.T, target[None], history.T)
    users = lax.all_to_all(columns, "items", split_axis=0, concat_axis=0, tiled=True).reshape(dim, u_dev)

    tiles = item_emb.reshape(item_dev // 8, 8, dim)
    rows = lambda n: jax.ShapeDtypeStruct((n, dim), jnp.bfloat16)
    fetched = lambda n: pltpu.VMEM((n, 8, dim), jnp.bfloat16)
    trow, hrow_a, notes, past = pl.pallas_call(
        target_kernel,
        out_shape=(
            rows(u_dev),
            rows(early_users),
            jax.ShapeDtypeStruct((2, u_dev), f32),
            jax.ShapeDtypeStruct((2, u_dev), jnp.int32),
        ),
        in_specs=[smem, vmem, hbm],
        out_specs=(vmem, vmem, vmem, vmem),
        scratch_shapes=[
            fetched(u_dev),
            fetched(early_users),
            pltpu.SemaphoreType.DMA,
            pltpu.SemaphoreType.DMA,
        ],
        compiler_params=pltpu.CompilerParams(vmem_limit_bytes=44 * 1024 * 1024),
        name="target",
    )(table, table, tiles)

    spread = jax.ShapeDtypeStruct((n_items, 1, u_dev), f32)
    part_t, token = pl.pallas_call(
        tscore_kernel,
        out_shape=(spread, jax.ShapeDtypeStruct((8, 128), f32)),
        in_specs=[vmem] * 3,
        out_specs=(vmem, vmem),
        compiler_params=small,
        name="tscore",
    )(users, trow, notes)
    parts_t = lax.all_to_all(part_t, "items", split_axis=0, concat_axis=0, tiled=True)
    hrow_b, head = pl.pallas_call(
        history_kernel,
        out_shape=(rows(u_dev - early_users), jax.ShapeDtypeStruct((block_items // 8, 8, dim), jnp.bfloat16)),
        in_specs=[smem, vmem, vmem, hbm],
        out_specs=(vmem, vmem),
        scratch_shapes=[fetched(u_dev - early_users), pltpu.SemaphoreType.DMA, pltpu.SemaphoreType.DMA],
        compiler_params=pltpu.CompilerParams(vmem_limit_bytes=44 * 1024 * 1024),
        name="history",
    )(past, past, token, tiles)

    local = pl.pallas_call(
        count_kernel,
        out_shape=spread,
        in_specs=[vmem, vmem, vmem, vmem, vmem, hbm],
        out_specs=vmem,
        scratch_shapes=[
            pltpu.VMEM((3, block_items, dim), jnp.bfloat16),
            pltpu.VMEM((dim, u_dev), jnp.bfloat16),
            pltpu.VMEM((8, u_dev), f32),
            pltpu.VMEM((8, u_dev), f32),
            pltpu.VMEM((1, u_dev), f32),
            pltpu.SemaphoreType.DMA((3,)),
        ],
        compiler_params=pltpu.CompilerParams(
            vmem_limit_bytes=40 * 1024 * 1024,
        ),
        name="count",
    )(users, hrow_a, hrow_b, parts_t, head.reshape(block_items, dim), item_emb)

    parts = lax.all_to_all(local, "items", split_axis=0, concat_axis=0, tiled=True)
    log_rank, sums = pl.pallas_call(
        metric_kernel,
        out_shape=(jax.ShapeDtypeStruct((1, u_dev), f32), jax.ShapeDtypeStruct((n_users, 1, 128), f32)),
        in_specs=[vmem, vmem],
        out_specs=(vmem, vmem),
        compiler_params=small,
        name="metric",
    )(parts, notes)
    sums = lax.all_to_all(sums, "users", split_axis=0, concat_axis=0, tiled=True)
    metrics = jnp.sum(sums, axis=(0, 1))[:2] / (u_dev * n_users)
    return (log_rank[0], metrics)


def solution(mesh):
    return jax.shard_map(
        body,
        mesh=mesh,
        in_specs=(P("users", "items"), P("items", None), P("users"), P("users", None)),
        out_specs=(P("users"), P()),
        check_vma=False,
    )
```
